32 devices in a mesh: row: 2 (over y), col: 4 (over z), depth: 4 (over x, core).
Axes of the slice: x: 2, y: 2, z: 4, core: 2. Of those that a mesh axis runs over, the one named last changes fastest.
Arguments:
- matrix: float32 [8, 2, 512, 8192], P(None, 'row', None, ('col', 'depth')), as said below
Outputs:
- factored: float32 [8, 2, 512, 8192], P(None, 'row', None, ('col', 'depth'))
Inputs may be any that keep to these rules, and one draw needn't show every extreme that they name: matrix is symmetric positive definite.
All inputs are finite; a program needn't handle non-finite values.
Results may differ from the reference program's by a relative error of at most 0.0001.
Values sent between devices are 32-bit elements; how exact they have to be, the bound alone decides.
A program may use at most 128 MiB of HBM per device.

```python
import math
import jax
import jax.numpy as jnp
from jax import lax

B = 512
PANELS = 2
RB = 8
NBLK = 16
ORDER = 8192
N_ROW = 2


def draw_matrix(key, part):
    key_normal = jax.random.fold_in(key, 11)
    key_diagonal = jax.random.fold_in(key, 12)
    latent = 4 * B
    gaussian = jax.random.normal(key_normal, (ORDER, latent), jnp.float32)
    product = jnp.dot(gaussian, gaussian.T, precision=lax.Precision.HIGHEST) / math.sqrt(latent)
    symmetric = (product + product.T) * 0.5
    diag_shift = jax.random.uniform(key_diagonal, (ORDER,), jnp.float32, 0.1, 0.3) * math.sqrt(latent)
    positions = jnp.arange(ORDER)
    symmetric = symmetric.at[positions, positions].add(diag_shift)
    return symmetric.reshape(RB, N_ROW, B, ORDER)


def setup_inputs(seed: int = 0) -> dict:
    seeds = jax.random.split(jax.random.key(seed), 2)
    return {
        "matrix": draw_matrix(jax.random.fold_in(seeds[1], 71), 0),
    }


def factor_blocks(lower_factor, blocks, block_ids, panel_index):
    count_rows, block_size, _ = blocks.shape
    solved = lax.linalg.triangular_solve(lower_factor, blocks.reshape(count_rows * block_size, block_size), left_side=False, lower=True, transpose_a=True)
    solved = solved.reshape(count_rows, block_size, block_size)
    marks = block_ids[:, None, None]
    return jnp.where(marks > panel_index, solved, jnp.where(marks == panel_index, lower_factor[None], jnp.float32(0.0)))

def reference(matrix):
    matrix_full = matrix.reshape(ORDER, ORDER)
    for panel_index in range(PANELS):
        start_col = panel_index * B
        stop_col = start_col + B
        lower_factor = jnp.linalg.cholesky(matrix_full[start_col:stop_col, start_col:stop_col])
        blocks = matrix_full[:, start_col:stop_col].reshape(NBLK, B, B)
        panel_full = factor_blocks(lower_factor, blocks, jnp.arange(NBLK, dtype=jnp.int32), panel_index).reshape(ORDER, B)
        trailing = matrix_full[:, stop_col:] - jnp.dot(panel_full, panel_full[stop_col:].T, precision=lax.Precision.HIGHEST)
        below_rows = (jnp.arange(ORDER, dtype=jnp.int32) >= stop_col)[:, None]
        trailing = jnp.where(below_rows, trailing, jnp.float32(0.0))
        matrix_full = jnp.concatenate([matrix_full[:, :start_col], panel_full, trailing], axis=1)
    return matrix_full.reshape(RB, N_ROW, B, ORDER)
```

```python
import functools

import jax
import jax.numpy as jnp
from jax import lax
from jax.experimental import pallas as pl
from jax.experimental.pallas import tpu as pltpu
from jax.sharding import PartitionSpec as P

PANELS = 2
MESH = pl.DeviceIdType.MESH
HI = lax.Precision.HIGHEST
T = 128
NT = (((1,), (1,)), ((), ()))
TN = (((0,), (0,)), ((), ()))
NN = (((1,), (0,)), ((), ()))
DIAGS = ((0, 0), (0, 1), (1, 1))


def dot(a, b, dims=NN):
    return lax.dot_general(a, b, dims, precision=HI, preferred_element_type=jnp.float32)


def factor_tile(aug, tick):
    def strip(i, carry):
        j0 = pl.multiple_of(i * 8, 8)
        rows = aug[pl.ds(j0, 8), :]
        lane = lax.broadcasted_iota(jnp.int32, (8, T), 1)
        sub = lax.broadcasted_iota(jnp.int32, (8, T), 0)
        sub2 = lax.broadcasted_iota(jnp.int32, (8, 2 * T), 0)
        left = rows[:, :T]
        cols = [
            jnp.broadcast_to(
                jnp.sum(jnp.where(lane == j0 + t, left, 0.0), axis=1, keepdims=True), (8, T)
            )
            for t in range(8)
        ]
        for t in range(8):
            p = cols[t][t : t + 1, :]
            r = lax.rsqrt(p)
            r = r * (1.5 - 0.5 * p * r * r)
            coef = cols[t] * r
            for u in range(t + 1, 8):
                head = cols[u][t : t + 1, :] * r
                cols[u] = jnp.where(sub > t, cols[u] - coef * head, cols[u])
            wide_r = jnp.concatenate([r, r], axis=1)
            wide_c = jnp.concatenate([coef, coef], axis=1)
            head = rows[t : t + 1, :] * wide_r
            rows = jnp.where(sub2 == t, head, jnp.where(sub2 > t, rows - wide_c * head, rows))
        aug[pl.ds(j0, 8), :] = rows
        later = jnp.where(lane >= j0 + 8, rows[:, :T], 0.0)
        aug[...] -= dot(later, rows, TN)
        return carry

    lax.fori_loop(0, T // 8, strip, 0)


def gather_kernel(
    shape, first, m_ref, x0_ref, x1_ref, cross_ref, w_ref, u_ref,
    diag, work, aug, dsend, drecv, dloc, xsend, xrecv, xloc, csend, crecv, cloc,
):
    n_row, n_col, n_dep = shape
    slots, block, _ = m_ref.shape
    n_chunk = 2 * (slots - first)
    half = block // 2
    r = lax.axis_index("row")
    c = lax.axis_index("col")
    d = lax.axis_index("depth")
    across = lax.rem(d + n_dep // 2, n_dep)
    sib = d + 1 - 2 * lax.rem(d, 2)
    x_refs = (x0_ref, x1_ref)
    n_dc = block // T

    def dest(rr=None, cc=None, dd=None):
        return (r if rr is None else rr, c if cc is None else cc, d if dd is None else dd)

    def role(k):
        is_same = d == k
        is_xp = d == (k + n_dep // 2) % n_dep
        return is_same, is_xp

    def diag_copy(n, g, lane, to):
        part = diag.at[n, pl.ds(g * T, T), :]
        return pltpu.make_async_remote_copy(
            src_ref=part, dst_ref=part, send_sem=dsend.at[n, g, lane], recv_sem=drecv.at[n, g],
            device_id=to, device_id_type=MESH,
        )

    def diag_out(n):
        row, k = DIAGS[n]
        is_same, is_xp = role(k)
        root = is_same & (c == 0) & (r == row)
        out = [
            (is_same & (c < n_col - 1), dest(cc=lax.rem(c + 1, n_col))),
            (is_same, dest(dd=across)),
            (is_same | is_xp, dest(dd=sib)),
        ]
        for step in range(1, n_row):
            out.append((root, dest(rr=lax.rem(r + step, n_row))))
        return root, out

    def diag_load(n, g):
        return pltpu.make_async_copy(
            m_ref.at[0, pl.ds(g * T, T), :], diag.at[n, pl.ds(g * T, T), :], dloc.at[n, g]
        )

    def diag_step(n, g, wait):
        root, out = diag_out(n)

        @pl.when(root)
        def _():
            diag_load(n, g).wait()

        if wait:
            @pl.when(jnp.logical_not(root))
            def _():
                diag_copy(n, g, 0, dest(dd=sib)).wait_recv()

        order = out[3:] + out[:3]
        lanes = list(range(3, len(out))) + [0, 1, 2]
        for lane, (cond, to) in zip(lanes, order):
            @pl.when(cond)
            def _():
                diag_copy(n, g, lane, to).start()

    def diag_drain(n, g):
        _, out = diag_out(n)
        for lane, (cond, to) in enumerate(out):
            @pl.when(cond)
            def _():
                diag_copy(n, g, lane, to).wait_send()

    def x_part(ref, q, shift):
        return ref.at[q // 2 + shift, pl.ds(lax.rem(q, 2) * half, half), :]

    def x_copy(k, q, lane, to, root):
        dst = x_part(x_refs[k], q, 0)
        src = x_part(m_ref, q, first) if root else dst
        return pltpu.make_async_remote_copy(
            src_ref=src, dst_ref=dst, send_sem=xsend.at[k, q, lane], recv_sem=xrecv.at[k, q],
            device_id=to, device_id_type=MESH,
        )

    def x_local(k, q):
        return pltpu.make_async_copy(
            x_part(m_ref, q, first), x_part(x_refs[k], q, 0), xloc.at[k, q]
        )

    def x_out(k, q):
        is_same, is_xp = role(k)
        tree_a = lax.rem(q, 2) == 0
        tree_b = jnp.logical_not(tree_a)
        root = is_same & (c == 0)
        along = (c < n_col - 1) & ((is_same & tree_a) | (is_xp & tree_b))
        side = (
            (is_same & tree_a & (c >= 1))
            | (is_same & tree_b & (c == 0))
            | (is_xp & tree_b & (c >= 1))
        )
        back = is_xp & tree_a & (c == 1)
        return root, [
            (along, dest(cc=lax.rem(c + 1, n_col))),
            (side, dest(dd=across)),
            (is_same | is_xp, dest(dd=sib)),
            (back, dest(cc=jnp.zeros_like(c))),
        ]

    def x_send(k, q, as_root):
        root, out = x_out(k, q)
        for lane, (cond, to) in enumerate(out):
            @pl.when(cond & (root if as_root else jnp.logical_not(root)))
            def _():
                x_copy(k, q, lane, to, as_root).start()

    def x_tick(q):
        for k in range(PANELS):
            root, _ = x_out(k, q)

            @pl.when(jnp.logical_not(root))
            def _():
                x_copy(k, q, 0, dest(dd=sib), False).wait_recv()
                x_send(k, q, False)

    def x_drain(q):
        for k in range(PANELS):
            root, out = x_out(k, q)
            for lane, (cond, to) in enumerate(out):
                @pl.when(cond)
                def _():
                    x_copy(k, q, lane, to, False).wait_send()

            @pl.when(root)
            def _():
                x_local(k, q).wait()

    def cross_copy(k, step):
        return pltpu.make_async_remote_copy(
            src_ref=m_ref.at[0], dst_ref=cross_ref.at[k], send_sem=csend.at[k, step - 1],
            recv_sem=crecv.at[k], device_id=dest(rr=lax.rem(r + step, n_row)), device_id_type=MESH,
        )

    def cross_local(k):
        return pltpu.make_async_copy(m_ref.at[0], cross_ref.at[k], cloc.at[k])

    for n, (row, k) in enumerate(DIAGS):
        @pl.when((d == k) & (c == 0) & (r == row))
        def _():
            for g in range(n_dc):
                diag_load(n, g).start()
    for g in range(n_dc):
        diag_step(0, g, True)
    for n in (1, 2):
        root, _ = diag_out(n)

        @pl.when(root)
        def _():
            for g in range(n_dc):
                diag_step(n, g, False)

    def send_all(q, carry):
        for k in range(PANELS):
            x_send(k, q, True)
            root, _ = x_out(k, q)

            @pl.when(root)
            def _():
                x_local(k, q).start()
        return carry

    lax.fori_loop(0, n_chunk, send_all, 0)
    for k in range(PANELS):
        @pl.when(r == k)
        def _():
            cross_local(k).start()
            for step in range(1, n_row):
                cross_copy(k, step).start()

    def diag_late(n):
        root, _ = diag_out(n)

        @pl.when(jnp.logical_not(root))
        def _():
            for g in range(n_dc):
                diag_step(n, g, True)

    def eye(rows, columns, at):
        i = lax.broadcasted_iota(jnp.int32, (rows, columns), 0)
        j = lax.broadcasted_iota(jnp.int32, (rows, columns), 1)
        return jnp.where(i + at == j, jnp.float32(1.0), jnp.float32(0.0))

    per = -(-n_chunk // (PANELS * n_dc))

    def factor_block(panel):
        def tile(b, carry):
            at = pl.multiple_of(b * T, T)
            aug[:, :T] = work[pl.ds(at, T), pl.ds(at, T)]
            aug[:, T:] = eye(T, T, 0)
            factor_tile(aug, None)
            line = dot(aug[:, T:], work[pl.ds(at, T), :])
            work[pl.ds(at, T), :] = line
            lane = lax.broadcasted_iota(jnp.int32, (T, block), 1)
            aside = jnp.where(lane >= at + T, line[:, :block], 0.0)

            def tail(e, carry2):
                cols = pl.ds(pl.multiple_of(e * 2 * T, 2 * T), 2 * T)
                work[:, cols] -= dot(aside, work[pl.ds(at, T), cols], TN)
                return carry2

            lax.fori_loop(0, block // T, tail, 0)

            for e in range(per):
                q = (panel * n_dc + b) * per + e

                @pl.when(q < n_chunk)
                def _():
                    x_tick(jnp.minimum(q, n_chunk - 1))
            return carry

        lax.fori_loop(0, n_dc, tile, 0)

    def upper(x, at):
        i = lax.broadcasted_iota(jnp.int32, x.shape, 0)
        j = lax.broadcasted_iota(jnp.int32, x.shape, 1)
        return jnp.where(i + at <= j, x, 0.0)

    def lower(x, at):
        i = lax.broadcasted_iota(jnp.int32, x.shape, 0)
        j = lax.broadcasted_iota(jnp.int32, x.shape, 1)
        return jnp.where(i + at >= j, x, 0.0)

    def each_tile(f):
        def step(e, carry):
            f(pl.multiple_of(e * T, T))
            return carry

        lax.fori_loop(0, block // T, step, 0)

    def fill(n):
        def f(at):
            rows = pl.ds(at, T)
            work[rows, :block] = diag[n, rows, :]
            work[rows, block:] = eye(T, block, at)
        return f

    def keep(base):
        def f(at):
            rows = pl.ds(at, T)
            to = pl.ds(base + at, T)
            u_ref[to, base : base + block] = upper(work[rows, :block], at)
            w_ref[to, base : base + block] = lower(work[rows, block:], at)
        return f

    each_tile(fill(0))
    factor_block(0)
    each_tile(keep(0))
    diag_late(1)
    diag_late(2)

    def join(at):
        rows = pl.ds(at, T)
        u_ref[rows, block:] = dot(w_ref[rows, :block], diag[1])
        w_ref[rows, block:] = jnp.zeros((T, block), jnp.float32)
        u_ref[pl.ds(block + at, T), :block] = jnp.zeros((T, block), jnp.float32)

    each_tile(join)

    def second(at):
        rows = pl.ds(at, T)
        cols = pl.ds(block + at, T)
        top = u_ref[:block, block:]
        work[rows, :block] = diag[2, rows, :] - dot(u_ref[:block, cols], top, TN)
        work[rows, block:] = eye(T, block, at)

    each_tile(second)
    factor_block(1)
    each_tile(keep(block))

    def below(at):
        rows = pl.ds(at, T)
        cols = pl.ds(block + at, T)
        work[rows, :block] = dot(u_ref[:block, cols], w_ref[:block, :block], TN)

    each_tile(below)

    def corner(at):
        rows = pl.ds(block + at, T)
        w_ref[rows, :block] = -dot(w_ref[rows, block:], work[:, :block])

    each_tile(corner)

    for k in range(PANELS):
        @pl.when(r == k)
        def _():
            cross_local(k).wait()
            for step in range(1, n_row):
                cross_copy(k, step).wait_send()

        @pl.when(r != k)
        def _():
            cross_copy(k, 1).wait_recv()
    for n in range(len(DIAGS)):
        for g in range(n_dc):
            diag_drain(n, g)

    def drain(q, carry):
        x_drain(q)
        return carry

    lax.fori_loop(0, n_chunk, drain, 0)


def split(x):
    top = x.astype(jnp.bfloat16)
    return top, (x - top.astype(jnp.float32)).astype(jnp.bfloat16)


def update_kernel(first, keep_ref, m_ref, x0_ref, x1_ref, mat_ref, fix_ref, o_ref, top, low):
    s = pl.program_id(0)
    block = o_ref.shape[-1]

    @pl.when(s == 0)
    def _():
        for k in range(PANELS):
            a, b = split(mat_ref[k * block : (k + 1) * block, :])
            top[k] = a
            low[k] = b

    def go():
        base = jnp.where(keep_ref[0] > 0, m_ref[0], 0.0)
        acc = base
        for k, x_ref in enumerate((x0_ref, x1_ref)):
            a, b = split(x_ref[0])
            for left, right in ((a, top), (a, low), (b, top)):
                acc = acc - jnp.dot(left, right[k], preferred_element_type=jnp.float32)
        return acc

    if first:
        @pl.when(s == 0)
        def _():
            o_ref[0] = fix_ref[...]

        @pl.when(s > 0)
        def _():
            o_ref[0] = go()
    else:
        o_ref[0] = go()

        @pl.when((s == 0) & (keep_ref[1] > 0))
        def _():
            o_ref[0] = fix_ref[...]


def body(shape, matrix):
    n_row, n_col, n_dep = shape
    m = matrix.reshape(matrix.shape[0], matrix.shape[2], matrix.shape[3])
    slots, block, _ = m.shape
    order = PANELS * block
    first = 1 if n_row <= PANELS else 0
    n_chunk = 2 * (slots - first)
    n_dc = block // T
    f32 = jnp.float32
    dma = pltpu.SemaphoreType.DMA
    hbm = pl.BlockSpec(memory_space=pltpu.HBM)
    vmem = pl.BlockSpec(memory_space=pltpu.VMEM)
    panel = jax.ShapeDtypeStruct((slots - first, block, block), f32)
    x0, x1, cross, w, u = pl.pallas_call(
        functools.partial(gather_kernel, shape, first),
        out_shape=(
            panel, panel,
            jax.ShapeDtypeStruct((PANELS, block, block), f32),
            jax.ShapeDtypeStruct((order, order), f32),
            jax.ShapeDtypeStruct((order, order), f32),
        ),
        in_specs=[hbm],
        out_specs=(hbm, hbm, hbm, vmem, vmem),
        scratch_shapes=[
            pltpu.VMEM((len(DIAGS), block, block), f32),
            pltpu.VMEM((block, 2 * block), f32),
            pltpu.VMEM((T, 2 * T), f32),
            dma((len(DIAGS), n_dc, 2 + n_row)),
            dma((len(DIAGS), n_dc)),
            dma((len(DIAGS), n_dc)),
            dma((PANELS, n_chunk, 4)),
            dma((PANELS, n_chunk)),
            dma((PANELS, n_chunk)),
            dma((PANELS, n_row - 1)),
            dma((PANELS,)),
            dma((PANELS,)),
        ],
        compiler_params=pltpu.CompilerParams(has_side_effects=True, vmem_limit_bytes=48 << 20),
    )(m)

    j = lax.axis_index(("col", "depth"))
    r = lax.axis_index("row")
    own = cross.reshape(order, block)
    solved = jnp.dot(w, own, precision=HI)
    i1 = lax.broadcasted_iota(jnp.int32, (order, block), 0)
    i2 = lax.broadcasted_iota(jnp.int32, (order, block), 1)
    unit = jnp.where(i1 == i2 + j * block, f32(-1.0), f32(0.0))
    mat = lax.dot_general(w, jnp.where(j < PANELS, unit, solved), TN, precision=HI)
    rr = jnp.minimum(r, PANELS - 1)
    jj = jnp.minimum(j, PANELS - 1)
    fix = lax.dynamic_slice(u, (jj * block, rr * block), (block, block)).T
    fix = jnp.where(j < PANELS, fix, f32(0.0))
    flags = jnp.stack([j >= PANELS, r < PANELS]).astype(jnp.int32)

    one = (1, block, block)
    shifted = lambda s: (jnp.maximum(s - first, 0), 0, 0)
    out = pl.pallas_call(
        functools.partial(update_kernel, first),
        out_shape=jax.ShapeDtypeStruct(m.shape, f32),
        grid=(slots,),
        in_specs=[
            pl.BlockSpec(memory_space=pltpu.SMEM),
            pl.BlockSpec(one, lambda s: (s, 0, 0)),
            pl.BlockSpec(one, shifted),
            pl.BlockSpec(one, shifted),
            pl.BlockSpec((order, block), lambda s: (0, 0)),
            pl.BlockSpec((block, block), lambda s: (0, 0)),
        ],
        out_specs=pl.BlockSpec(one, lambda s: (s, 0, 0)),
        scratch_shapes=[
            pltpu.VMEM((PANELS, block, block), jnp.bfloat16),
            pltpu.VMEM((PANELS, block, block), jnp.bfloat16),
        ],
        compiler_params=pltpu.CompilerParams(vmem_limit_bytes=40 << 20),
    )(flags, m, x0, x1, mat, fix)
    return out.reshape(matrix.shape)


def solution(mesh):
    shape = (mesh.shape["row"], mesh.shape["col"], mesh.shape["depth"])
    placed = P(None, "row", None, ("col", "depth"))
    return jax.shard_map(
        functools.partial(body, shape),
        mesh=mesh,
        in_specs=(placed,),
        out_specs=placed,
        check_vma=False,
    )
```

```python
import functools

import jax
import jax.numpy as jnp
from jax import lax
from jax.experimental import pallas as pl
from jax.experimental.pallas import tpu as pltpu
from jax.sharding import PartitionSpec as P

PANELS = 2
MESH = pl.DeviceIdType.MESH
HI = lax.Precision.HIGHEST
T = 128
NT = (((1,), (1,)), ((), ()))
TN = (((0,), (0,)), ((), ()))
NN = (((1,), (0,)), ((), ()))
DIAGS = ((0, 0), (0, 1), (1, 1))


def dot(a, b, dims=NN):
    return lax.dot_general(a, b, dims, precision=HI, preferred_element_type=jnp.float32)


def factor_tile(aug, tick):
    def strip(i, carry):
        j0 = pl.multiple_of(i * 8, 8)
        rows = aug[pl.ds(j0, 8), :]
        lane = lax.broadcasted_iota(jnp.int32, (8, T), 1)
        sub = lax.broadcasted_iota(jnp.int32, (8, T), 0)
        sub2 = lax.broadcasted_iota(jnp.int32, (8, 2 * T), 0)
        left = rows[:, :T]
        cols = [
            jnp.broadcast_to(
                jnp.sum(jnp.where(lane == j0 + t, left, 0.0), axis=1, keepdims=True), (8, T)
            )
            for t in range(8)
        ]
        for t in range(8):
            p = cols[t][t : t + 1, :]
            r = lax.rsqrt(p)
            r = r * (1.5 - 0.5 * p * r * r)
            coef = cols[t] * r
            for u in range(t + 1, 8):
                head = cols[u][t : t + 1, :] * r
                cols[u] = jnp.where(sub > t, cols[u] - coef * head, cols[u])
            wide_r = jnp.concatenate([r, r], axis=1)
            wide_c = jnp.concatenate([coef, coef], axis=1)
            head = rows[t : t + 1, :] * wide_r
            rows = jnp.where(sub2 == t, head, jnp.where(sub2 > t, rows - wide_c * head, rows))
        aug[pl.ds(j0, 8), :] = rows
        later = jnp.where(lane >= j0 + 8, rows[:, :T], 0.0)
        aug[...] -= dot(later, rows, TN)

        @pl.when(lax.rem(i, 4) == 3)
        def _():
            tick(i // 4)
        return carry

    lax.fori_loop(0, T // 8, strip, 0)


def gather_kernel(
    shape, first, m_ref, x0_ref, x1_ref, cross_ref, w_ref, u_ref,
    diag, work, aug, dsend, drecv, dloc, xsend, xrecv, xloc, csend, crecv, cloc,
):
    n_row, n_col, n_dep = shape
    slots, block, _ = m_ref.shape
    n_chunk = 2 * (slots - first)
    half = block // 2
    r = lax.axis_index("row")
    c = lax.axis_index("col")
    d = lax.axis_index("depth")
    across = lax.rem(d + n_dep // 2, n_dep)
    sib = d + 1 - 2 * lax.rem(d, 2)
    x_refs = (x0_ref, x1_ref)
    n_dc = block // T

    def dest(rr=None, cc=None, dd=None):
        return (r if rr is None else rr, c if cc is None else cc, d if dd is None else dd)

    def role(k):
        is_same = d == k
        is_xp = d == (k + n_dep // 2) % n_dep
        return is_same, is_xp

    def hop_of(k):
        return jnp.where(lax.rem(d, 2) == k % 2, 0, 1)

    def diag_copy(n, g, lane, to):
        part = diag.at[n, pl.ds(g * T, T), :]
        return pltpu.make_async_remote_copy(
            src_ref=part, dst_ref=part, send_sem=dsend.at[n, g, lane], recv_sem=drecv.at[n, g],
            device_id=to, device_id_type=MESH,
        )

    def diag_out(n):
        row, k = DIAGS[n]
        is_same, is_xp = role(k)
        root = is_same & (c == 0) & (r == row)
        out = [
            (is_same & (c < n_col - 1), dest(cc=lax.rem(c + 1, n_col))),
            (is_same, dest(dd=across)),
            (is_same | is_xp, dest(dd=sib)),
        ]
        for step in range(1, n_row):
            out.append((root, dest(rr=lax.rem(r + step, n_row))))
        return root, out

    def diag_load(n, g):
        return pltpu.make_async_copy(
            m_ref.at[0, pl.ds(g * T, T), :], diag.at[n, pl.ds(g * T, T), :], dloc.at[n, g]
        )

    def diag_step(n, g, wait):
        root, out = diag_out(n)

        @pl.when(root)
        def _():
            diag_load(n, g).wait()

        if wait:
            @pl.when(jnp.logical_not(root))
            def _():
                diag_copy(n, g, 0, dest(dd=sib)).wait_recv()

        order = out[3:] + out[:3]
        lanes = list(range(3, len(out))) + [0, 1, 2]
        for lane, (cond, to) in zip(lanes, order):
            @pl.when(cond)
            def _():
                diag_copy(n, g, lane, to).start()

    def diag_drain(n, g):
        _, out = diag_out(n)
        for lane, (cond, to) in enumerate(out):
            @pl.when(cond)
            def _():
                diag_copy(n, g, lane, to).wait_send()

    def x_part(ref, q, shift):
        return ref.at[q // 2 + shift, pl.ds(lax.rem(q, 2) * half, half), :]

    def x_copy(k, q, lane, to, root):
        dst = x_part(x_refs[k], q, 0)
        src = x_part(m_ref, q, first) if root else dst
        return pltpu.make_async_remote_copy(
            src_ref=src, dst_ref=dst, send_sem=xsend.at[k, q, lane], recv_sem=xrecv.at[k, q],
            device_id=to, device_id_type=MESH,
        )

    def x_local(k, q):
        return pltpu.make_async_copy(
            x_part(m_ref, q, first), x_part(x_refs[k], q, 0), xloc.at[k, q]
        )

    def x_out(k, q):
        is_same, is_xp = role(k)
        tree_a = lax.rem(q, 2) == 0
        tree_b = jnp.logical_not(tree_a)
        root = is_same & (c == 0)
        along = (c < n_col - 1) & ((is_same & tree_a) | (is_xp & tree_b))
        side = (
            (is_same & tree_a & (c >= 1))
            | (is_same & tree_b & (c == 0))
            | (is_xp & tree_b & (c >= 1))
        )
        back = is_xp & tree_a & (c == 1)
        return root, [
            (along, dest(cc=lax.rem(c + 1, n_col))),
            (side, dest(dd=across)),
            (is_same | is_xp, dest(dd=sib)),
            (back, dest(cc=jnp.zeros_like(c))),
        ]

    def x_send(k, q, as_root):
        root, out = x_out(k, q)
        for lane, (cond, to) in enumerate(out):
            @pl.when(cond & (root if as_root else jnp.logical_not(root)))
            def _():
                x_copy(k, q, lane, to, as_root).start()

    def tick(t):
        for n in (1, 2):
            row, k = DIAGS[n]
            near = (d - lax.rem(d, 2)) == (k - k % 2)
            hops = c + hop_of(k) + jnp.where(near, 0, 1) + jnp.where(r == row, 0, 1)
            root, _ = diag_out(n)
            e = t - hops
            g = jnp.minimum(jnp.maximum(e, 0), n_dc - 1)

            @pl.when(jnp.logical_not(root) & (e >= 0) & (e < n_dc))
            def _():
                diag_step(n, g, True)
        for k in range(PANELS):
            is_same, is_xp = role(k)
            sib_hop = hop_of(k)
            near = (d - lax.rem(d, 2)) == (k - k % 2)
            for tree in range(2):
                if tree == 0:
                    far = jnp.where(c == 0, 3, c + 1)
                    hops = jnp.where(near, c, far) + sib_hop
                else:
                    back = jnp.where(c == 0, 0, c + 2)
                    hops = jnp.where(near, back, c + 1) + sib_hop
                e = t - 2 * hops
                q = jnp.minimum(jnp.maximum(e, 0), n_chunk - 1)
                root = is_same & (c == 0)
                now = (e >= 0) & (e < n_chunk) & (lax.rem(q, 2) == tree)

                @pl.when(now & jnp.logical_not(root))
                def _():
                    x_copy(k, q, 0, dest(dd=sib), False).wait_recv()
                    x_send(k, q, False)

    def x_drain(q):
        for k in range(PANELS):
            root, out = x_out(k, q)
            for lane, (cond, to) in enumerate(out):
                @pl.when(cond)
                def _():
                    x_copy(k, q, lane, to, False).wait_send()

            @pl.when(root)
            def _():
                x_local(k, q).wait()

    def cross_copy(k, step):
        return pltpu.make_async_remote_copy(
            src_ref=m_ref.at[0], dst_ref=cross_ref.at[k], send_sem=csend.at[k, step - 1],
            recv_sem=crecv.at[k], device_id=dest(rr=lax.rem(r + step, n_row)), device_id_type=MESH,
        )

    def cross_local(k):
        return pltpu.make_async_copy(m_ref.at[0], cross_ref.at[k], cloc.at[k])

    for n, (row, k) in enumerate(DIAGS):
        @pl.when((d == k) & (c == 0) & (r == row))
        def _():
            for g in range(n_dc):
                diag_load(n, g).start()
    for g in range(n_dc):
        diag_step(0, g, True)
    for n in (1, 2):
        root, _ = diag_out(n)

        @pl.when(root)
        def _():
            for g in range(n_dc):
                diag_step(n, g, False)

    def send_all(q, carry):
        for k in range(PANELS):
            x_send(k, q, True)
            root, _ = x_out(k, q)

            @pl.when(root)
            def _():
                x_local(k, q).start()
        return carry

    lax.fori_loop(0, n_chunk, send_all, 0)
    for k in range(PANELS):
        @pl.when(r == k)
        def _():
            cross_local(k).start()
            for step in range(1, n_row):
                cross_copy(k, step).start()

    def eye(rows, columns, at):
        i = lax.broadcasted_iota(jnp.int32, (rows, columns), 0)
        j = lax.broadcasted_iota(jnp.int32, (rows, columns), 1)
        return jnp.where(i + at == j, jnp.float32(1.0), jnp.float32(0.0))

    n_tick = T // 32

    def factor_block(panel):
        def tile(b, carry):
            at = pl.multiple_of(b * T, T)
            aug[:, :T] = work[pl.ds(at, T), pl.ds(at, T)]
            aug[:, T:] = eye(T, T, 0)
            factor_tile(aug, lambda e: tick((panel * n_dc + b) * n_tick + e))
            line = dot(aug[:, T:], work[pl.ds(at, T), :])
            work[pl.ds(at, T), :] = line
            lane = lax.broadcasted_iota(jnp.int32, (T, block), 1)
            aside = jnp.where(lane >= at + T, line[:, :block], 0.0)

            def tail(e, carry2):
                cols = pl.ds(pl.multiple_of(e * 2 * T, 2 * T), 2 * T)
                work[:, cols] -= dot(aside, work[pl.ds(at, T), cols], TN)
                return carry2

            lax.fori_loop(0, block // T, tail, 0)
            return carry

        lax.fori_loop(0, n_dc, tile, 0)

    def upper(x, at):
        i = lax.broadcasted_iota(jnp.int32, x.shape, 0)
        j = lax.broadcasted_iota(jnp.int32, x.shape, 1)
        return jnp.where(i + at <= j, x, 0.0)

    def lower(x, at):
        i = lax.broadcasted_iota(jnp.int32, x.shape, 0)
        j = lax.broadcasted_iota(jnp.int32, x.shape, 1)
        return jnp.where(i + at >= j, x, 0.0)

    def each_tile(f):
        def step(e, carry):
            f(pl.multiple_of(e * T, T))
            return carry

        lax.fori_loop(0, block // T, step, 0)

    def fill(n):
        def f(at):
            rows = pl.ds(at, T)
            work[rows, :block] = diag[n, rows, :]
            work[rows, block:] = eye(T, block, at)
        return f

    def keep(base):
        def f(at):
            rows = pl.ds(at, T)
            to = pl.ds(base + at, T)
            u_ref[to, base : base + block] = upper(work[rows, :block], at)
            w_ref[to, base : base + block] = lower(work[rows, block:], at)
        return f

    each_tile(fill(0))
    factor_block(0)
    each_tile(keep(0))

    def join(at):
        rows = pl.ds(at, T)
        u_ref[rows, block:] = dot(w_ref[rows, :block], diag[1])
        w_ref[rows, block:] = jnp.zeros((T, block), jnp.float32)
        u_ref[pl.ds(block + at, T), :block] = jnp.zeros((T, block), jnp.float32)

    each_tile(join)

    def second(at):
        rows = pl.ds(at, T)
        cols = pl.ds(block + at, T)
        top = u_ref[:block, block:]
        work[rows, :block] = diag[2, rows, :] - dot(u_ref[:block, cols], top, TN)
        work[rows, block:] = eye(T, block, at)

    each_tile(second)
    factor_block(1)
    each_tile(keep(block))

    def below(at):
        rows = pl.ds(at, T)
        cols = pl.ds(block + at, T)
        work[rows, :block] = dot(u_ref[:block, cols], w_ref[:block, :block], TN)

    each_tile(below)

    def corner(at):
        rows = pl.ds(block + at, T)
        w_ref[rows, :block] = -dot(w_ref[rows, block:], work[:, :block])

    each_tile(corner)

    def rest(t, carry):
        tick(t)
        return carry

    lax.fori_loop(PANELS * n_dc * n_tick, max(n_chunk + 2 * (n_col + 2), 32), rest, 0)
    for k in range(PANELS):
        @pl.when(r == k)
        def _():
            cross_local(k).wait()
            for step in range(1, n_row):
                cross_copy(k, step).wait_send()

        @pl.when(r != k)
        def _():
            cross_copy(k, 1).wait_recv()
    for n in range(len(DIAGS)):
        for g in range(n_dc):
            diag_drain(n, g)

    def drain(q, carry):
        x_drain(q)
        return carry

    lax.fori_loop(0, n_chunk, drain, 0)


def split(x):
    top = x.astype(jnp.bfloat16)
    return top, (x - top.astype(jnp.float32)).astype(jnp.bfloat16)


def update_kernel(first, keep_ref, m_ref, x0_ref, x1_ref, mat_ref, fix_ref, o_ref, top, low):
    s = pl.program_id(0)
    block = o_ref.shape[-1]

    @pl.when(s == 0)
    def _():
        for k in range(PANELS):
            a, b = split(mat_ref[k * block : (k + 1) * block, :])
            top[k] = a
            low[k] = b

    def go():
        base = jnp.where(keep_ref[0] > 0, m_ref[0], 0.0)
        acc = base
        for k, x_ref in enumerate((x0_ref, x1_ref)):
            a, b = split(x_ref[0])
            for left, right in ((a, top), (a, low), (b, top)):
                acc = acc - jnp.dot(left, right[k], preferred_element_type=jnp.float32)
        return acc

    if first:
        @pl.when(s == 0)
        def _():
            o_ref[0] = fix_ref[...]

        @pl.when(s > 0)
        def _():
            o_ref[0] = go()
    else:
        o_ref[0] = go()

        @pl.when((s == 0) & (keep_ref[1] > 0))
        def _():
            o_ref[0] = fix_ref[...]


def body(shape, matrix):
    n_row, n_col, n_dep = shape
    m = matrix.reshape(matrix.shape[0], matrix.shape[2], matrix.shape[3])
    slots, block, _ = m.shape
    order = PANELS * block
    first = 1 if n_row <= PANELS else 0
    n_chunk = 2 * (slots - first)
    n_dc = block // T
    f32 = jnp.float32
    dma = pltpu.SemaphoreType.DMA
    hbm = pl.BlockSpec(memory_space=pltpu.HBM)
    vmem = pl.BlockSpec(memory_space=pltpu.VMEM)
    panel = jax.ShapeDtypeStruct((slots - first, block, block), f32)
    x0, x1, cross, w, u = pl.pallas_call(
        functools.partial(gather_kernel, shape, first),
        out_shape=(
            panel, panel,
            jax.ShapeDtypeStruct((PANELS, block, block), f32),
            jax.ShapeDtypeStruct((order, order), f32),
            jax.ShapeDtypeStruct((order, order), f32),
        ),
        in_specs=[hbm],
        out_specs=(hbm, hbm, hbm, vmem, vmem),
        scratch_shapes=[
            pltpu.VMEM((len(DIAGS), block, block), f32),
            pltpu.VMEM((block, 2 * block), f32),
            pltpu.VMEM((T, 2 * T), f32),
            dma((len(DIAGS), n_dc, 2 + n_row)),
            dma((len(DIAGS), n_dc)),
            dma((len(DIAGS), n_dc)),
            dma((PANELS, n_chunk, 4)),
            dma((PANELS, n_chunk)),
            dma((PANELS, n_chunk)),
            dma((PANELS, n_row - 1)),
            dma((PANELS,)),
            dma((PANELS,)),
        ],
        compiler_params=pltpu.CompilerParams(has_side_effects=True, vmem_limit_bytes=48 << 20),
    )(m)

    j = lax.axis_index(("col", "depth"))
    r = lax.axis_index("row")
    own = cross.reshape(order, block)
    solved = jnp.dot(w, own, precision=HI)
    i1 = lax.broadcasted_iota(jnp.int32, (order, block), 0)
    i2 = lax.broadcasted_iota(jnp.int32, (order, block), 1)
    unit = jnp.where(i1 == i2 + j * block, f32(-1.0), f32(0.0))
    mat = lax.dot_general(w, jnp.where(j < PANELS, unit, solved), TN, precision=HI)
    rr = jnp.minimum(r, PANELS - 1)
    jj = jnp.minimum(j, PANELS - 1)
    fix = lax.dynamic_slice(u, (jj * block, rr * block), (block, block)).T
    fix = jnp.where(j < PANELS, fix, f32(0.0))
    flags = jnp.stack([j >= PANELS, r < PANELS]).astype(jnp.int32)

    one = (1, block, block)
    shifted = lambda s: (jnp.maximum(s - first, 0), 0, 0)
    out = pl.pallas_call(
        functools.partial(update_kernel, first),
        out_shape=jax.ShapeDtypeStruct(m.shape, f32),
        grid=(slots,),
        in_specs=[
            pl.BlockSpec(memory_space=pltpu.SMEM),
            pl.BlockSpec(one, lambda s: (s, 0, 0)),
            pl.BlockSpec(one, shifted),
            pl.BlockSpec(one, shifted),
            pl.BlockSpec((order, block), lambda s: (0, 0)),
            pl.BlockSpec((block, block), lambda s: (0, 0)),
        ],
        out_specs=pl.BlockSpec(one, lambda s: (s, 0, 0)),
        scratch_shapes=[
            pltpu.VMEM((PANELS, block, block), jnp.bfloat16),
            pltpu.VMEM((PANELS, block, block), jnp.bfloat16),
        ],
        compiler_params=pltpu.CompilerParams(vmem_limit_bytes=40 << 20),
    )(flags, m, x0, x1, mat, fix)
    return out.reshape(matrix.shape)


def solution(mesh):
    shape = (mesh.shape["row"], mesh.shape["col"], mesh.shape["depth"])
    placed = P(None, "row", None, ("col", "depth"))
    return jax.shard_map(
        functools.partial(body, shape),
        mesh=mesh,
        in_specs=(placed,),
        out_specs=placed,
        check_vma=False,
    )
```
